128 devices in a mesh: replica: 8 (over z, core), tp: 16 (over y, x).
Axes of the slice: x: 4, y: 4, z: 4, core: 2. Of those that a mesh axis runs over, the one named last changes fastest.
Arguments:
- hidden: bfloat16 [1024, 8192], P(('replica', 'tp')), may hold values from -64 to 64
- head: bfloat16 [152064, 8192], P(('replica', 'tp'))
- token_ids: int32 [1024], replicated, may hold values from 0 to 152063
Outputs:
- logprob: float32 [1024], P(('replica', 'tp'))
The draws below stay inside these ranges and needn't reach their ends.
All inputs are finite; a program needn't handle non-finite values.
Results may differ from the reference program's by a relative error of at most 0.0003.
Values may be sent and summed in bfloat16 or wider, within the bound.
No kernel may reach another device: no remote copies, remote signals or barrier semaphores. Data moves between devices by JAX's collectives and lax.ppermute only.
A program may use at most 128 MiB of HBM per device.

```python
import math
import jax
import jax.numpy as jnp
from jax import lax

D = 8192
V = 152064
SEQS = 1024


def head_row(key, index):
    values = jax.random.normal(jax.random.fold_in(key, index), (D,), jnp.float32)
    return jnp.clip(values, -6.0, 6.0) * (3.0 / math.sqrt(D))


def head_rows(key, indices):
    base = jax.random.fold_in(key, 11)
    return jax.vmap(lambda index: head_row(base, index))(indices)


def draw_head(key, part):
    return head_rows(key, jnp.arange(V, dtype=jnp.int32)).astype(jnp.bfloat16)


def draw_hidden(key, part):
    drawn = jnp.clip(jax.random.normal(jax.random.fold_in(key, 21), (SEQS, D), jnp.float32), -6.0, 6.0)
    return drawn.astype(jnp.bfloat16)


def place_ends(result, rng, smallest, largest):
    index_at = [jax.random.randint(jax.random.fold_in(rng, axis), (), 0, length) for axis, length in enumerate(result.shape)]
    main_axis = result.shape.index(max(result.shape))
    beside = index_at[:main_axis] + [(index_at[main_axis] + 1) % result.shape[main_axis]] + index_at[main_axis + 1:]
    return result.at[tuple(index_at)].set(smallest).at[tuple(beside)].set(largest)


def setup_inputs(seed: int = 0) -> dict:
    key_list = jax.random.split(jax.random.key(seed), 4)
    return {
        "hidden": draw_hidden(jax.random.fold_in(key_list[3], 71), 0),
        "head": draw_head(jax.random.fold_in(key_list[3], 71), 0),
        "token_ids": place_ends(jax.random.randint(key_list[2], (SEQS,), 0, V), jax.random.fold_in(key_list[2], 1), 0, V - 1).astype(jnp.int32),
    }


def reference(hidden, head, token_ids):
    logits = lax.dot_general(hidden, head, (((1,), (1,)), ((), ())), preferred_element_type=jnp.float32)
    row_top = jnp.max(logits, axis=1)
    row_total = jnp.sum(jnp.exp(logits - row_top[:, None]), axis=1)
    row_picked = jnp.take_along_axis(logits, token_ids[:, None].astype(jnp.int32), axis=1)[:, 0]
    return row_picked - row_top - jnp.log(row_total)
```

```python
import jax
import jax.numpy as jnp
from jax import lax
from jax.sharding import PartitionSpec as P

AXES = ("replica", "tp")
FIRST, SECOND, THIRD = ("y", "x"), ("x", "z"), ("z", "y")
AHEAD, BEHIND, ACROSS = (1, -1), (-1, 1), (2, 2)


def device(z, core, y, x):
    return ((z % 4) * 2 + core) * 16 + (y % 4) * 4 + (x % 4)


def everyone():
    return [(z, c, y, x) for z in range(4) for c in range(2) for y in range(4) for x in range(4)]


def send(block, dims, hops):
    pairs = []
    for z, c, y, x in everyone():
        to = {"z": z, "y": y, "x": x}
        to[dims[c]] += hops[c]
        pairs.append((device(z, c, y, x), device(to["z"], c, to["y"], to["x"])))
    return lax.ppermute(block, AXES, pairs)


def to_partner(block):
    pairs = [(device(z, c, y, x), device(z, 1 - c, y, x)) for z, c, y, x in everyone()]
    return lax.ppermute(block, AXES, pairs)


def around(block, dims):
    got = [send(block, dims, hops) for hops in (AHEAD, BEHIND, ACROSS)]
    return jnp.concatenate([block] + got, axis=0)


def around_last(block, dims):
    half = block.shape[0] // 2
    left, right = send(block, dims, AHEAD), send(block, dims, BEHIND)
    far = [send(left[:half], dims, AHEAD), send(right[half:], dims, BEHIND)]
    return [block, left, right] + far


def shards(hidden, head, token_ids):
    rows = hidden.shape[0]
    vocab = head.shape[0]
    place, spot = lax.axis_index("replica"), lax.axis_index("tp")
    core = place % 2
    at = {"z": place // 2, "y": spot // 4, "x": spot % 4}

    other_head = to_partner(head)
    plane = around(around(hidden, FIRST), SECOND)
    gathered = jnp.concatenate(around_last(plane, THIRD), axis=0)

    slots = jnp.where(core == 0, jnp.array([0, 2, 3, 1], jnp.int32), jnp.array([0, 1, 3, 2], jnp.int32))
    offsets = jnp.where(core == 0, jnp.array([0, 3, 1, 2], jnp.int32), jnp.array([0, 1, 3, 2], jnp.int32))
    grid = jnp.arange(4, dtype=jnp.int32)

    def by_axis(axis, values):
        out = values[2]
        for phase, dims in ((0, FIRST), (1, SECOND)):
            hit = jnp.where(core == 0, dims[0] == axis, dims[1] == axis)
            out = jnp.where(hit, values[phase], out)
        return out

    strides = (1, 4, 16)
    block_of = jnp.zeros((4, 4, 4), jnp.int32)
    for n, axis in enumerate("zyx"):
        slot = slots[(grid - at[axis]) % 4] * by_axis(axis, strides)
        block_of = block_of + slot.reshape([4 if k == n else 1 for k in range(3)])
    block_of = block_of.reshape(64)
    number = jnp.arange(64, dtype=jnp.int32)
    steps = [number % 4, number // 4 % 4, number // 16]
    owner = jnp.zeros((64,), jnp.int32)
    for axis, stride in (("z", 16), ("y", 4), ("x", 1)):
        owner = owner + (at[axis] + offsets[by_axis(axis, steps)]) % 4 * stride
    tokens = token_ids.reshape(4, 2, 16, rows)
    tokens = lax.dynamic_index_in_dim(tokens, core, 1, keepdims=False).reshape(64, rows)
    tokens = tokens[owner].reshape(-1)

    position = place * 16 + spot
    other = (at["z"] * 2 + 1 - core) * 16 + spot
    tops, totals, picks = [], [], []
    for part, which in ((head, position), (other_head, other)):
        logits = lax.dot_general(gathered, part, (((1,), (1,)), ((), ())), preferred_element_type=jnp.float32)
        columns = which * vocab + jnp.arange(vocab, dtype=jnp.int32)
        top = jnp.max(logits, axis=1)
        tops.append(top)
        totals.append(jnp.sum(jnp.exp(logits - top[:, None]), axis=1))
        picks.append(jnp.sum(jnp.where(columns[None, :] == tokens[:, None], logits, 0.0), axis=1))
    top = jnp.maximum(*tops)
    total = totals[0] * jnp.exp(tops[0] - top) + totals[1] * jnp.exp(tops[1] - top)
    spread = (top + jnp.log(total)).reshape(64, rows)
    picked = (picks[0] + picks[1]).reshape(64, rows)
    stats = jnp.concatenate([spread, picked], axis=1)[block_of]

    groups = [[device(z, c, y, x) for z in range(4) for y in range(4) for x in range(4)] for c in range(2)]
    arrived = lax.all_to_all(stats, AXES, 0, 0, tiled=True, axis_index_groups=groups)
    spread, picked = arrived[:, :rows], jnp.sum(arrived[:, rows:], axis=0)
    top = jnp.max(spread, axis=0)
    return picked - top - jnp.log(jnp.sum(jnp.exp(spread - top[None, :]), axis=0))


def solution(mesh):
    in_specs = (P(AXES, None), P(AXES, None), P())
    return jax.shard_map(shards, mesh=mesh, in_specs=in_specs, out_specs=P(AXES), check_vma=False)
```

```python
import functools

import jax
import jax.numpy as jnp
import numpy as np
from jax import lax
from jax.experimental import pallas as pl
from jax.experimental.pallas import tpu as pltpu
from jax.sharding import PartitionSpec as P

AXES = ("replica", "tp")
FIRST, SECOND, THIRD = ("y", "x"), ("x", "z"), ("z", "y")
AHEAD, BEHIND, ACROSS = (1, -1), (-1, 1), (2, 2)
SLAB, SLOTS = 1024, 4


def device(z, core, y, x):
    return ((z % 4) * 2 + core) * 16 + (y % 4) * 4 + (x % 4)


def everyone():
    return [(z, c, y, x) for z in range(4) for c in range(2) for y in range(4) for x in range(4)]


def moved(z, c, y, x, dims, hops):
    to = {"z": z, "y": y, "x": x}
    to[dims[c]] += hops[c]
    return to["z"] % 4, c, to["y"] % 4, to["x"] % 4


def arrival_tables():
    started = np.zeros((128, 64), np.int32)
    arrives = np.zeros((128, 64), np.int32)
    back = [(0, 0), BEHIND, AHEAD, ACROSS]
    for me in everyone():
        for block in range(64):
            at = me
            for dims, slot in ((THIRD, block // 16), (SECOND, block // 4 % 4), (FIRST, block % 4)):
                at = moved(*at, dims, back[slot])
            z, _, y, x = at
            started[device(*me), block] = device(*at)
            arrives[device(*me), z * 16 + y * 4 + x] = block
    return started, arrives


def send(block, dims, hops):
    pairs = [(device(*me), device(*moved(*me, dims, hops))) for me in everyone()]
    return lax.ppermute(block, AXES, pairs)


def to_partner(block):
    pairs = [(device(z, c, y, x), device(z, 1 - c, y, x)) for z, c, y, x in everyone()]
    return lax.ppermute(block, AXES, pairs)


def around(block, dims):
    got = [send(block, dims, hops) for hops in (AHEAD, BEHIND, ACROSS)]
    return jnp.concatenate([block] + got, axis=0)


def together(*values):
    return lax.optimization_barrier(values)


def row_stats_kernel(sizes, wanted_ref, *refs):
    pieces = refs[: len(sizes)]
    mine_ref, other_ref, out_ref, rows_ref, slab_ref, logits_ref, row_sems, slab_sems = refs[len(sizes) :]
    width = mine_ref.shape[1]
    slabs = width // SLAB

    def fetch_rows(n):
        start, copies = 0, []
        for k, (size, piece) in enumerate(zip(sizes, pieces)):
            source = piece.at[:, pl.ds(n * SLAB, SLAB)]
            copies.append(pltpu.make_async_copy(source, rows_ref.at[n, pl.ds(start, size)], row_sems.at[k, n]))
            start += size
        return copies

    def fetch_slab(head_ref, n, slot):
        source = head_ref.at[:, pl.ds(pl.multiple_of(n * SLAB, SLAB), SLAB)]
        return pltpu.make_async_copy(source, slab_ref.at[slot], slab_sems.at[slot])

    for n in range(slabs):
        if n < SLOTS - 1:
            fetch_slab(mine_ref, n, n).start()
        for copy in fetch_rows(n):
            copy.start()

    for half, head_ref in enumerate((mine_ref, other_ref)):

        def step(n, _):
            turn = half * slabs + n
            slot = lax.rem(turn, SLOTS)
            ahead = n + SLOTS - 1
            free = lax.rem(turn + SLOTS - 1, SLOTS)

            @pl.when(ahead < slabs)
            def _():
                fetch_slab(head_ref, ahead, free).start()

            if half == 0:

                @pl.when(ahead >= slabs)
                def _():
                    fetch_slab(other_ref, ahead - slabs, free).start()

                start = 0
                for k, (size, piece) in enumerate(zip(sizes, pieces)):
                    source = piece.at[:, pl.ds(pl.multiple_of(n * SLAB, SLAB), SLAB)]
                    pltpu.make_async_copy(source, rows_ref.at[n, pl.ds(start, size)], row_sems.at[k, n]).wait()
                    start += size

            fetch_slab(head_ref, n, slot).wait()
            product = lax.dot_general(
                slab_ref[slot], rows_ref[n], (((1,), (1,)), ((), ())), preferred_element_type=jnp.float32
            )

            @pl.when(n == 0)
            def _():
                logits_ref[half] = product

            @pl.when(n > 0)
            def _():
                logits_ref[half] += product

            return 0

        lax.fori_loop(0, slabs, step, 0)

    top = jnp.maximum(
        jnp.max(logits_ref[0], axis=0, keepdims=True), jnp.max(logits_ref[1], axis=0, keepdims=True)
    )
    entry = lax.broadcasted_iota(jnp.int32, logits_ref.shape[1:], 0)
    total, picked = jnp.zeros_like(top), jnp.zeros_like(top)
    for half in range(2):
        logits = logits_ref[half]
        total += jnp.sum(jnp.exp(logits - top), axis=0, keepdims=True)
        hit = entry == wanted_ref[half : half + 1, :]
        picked += jnp.sum(jnp.where(hit, logits, 0.0), axis=0, keepdims=True)
    out_ref[0:1, :] = top + jnp.log(total)
    out_ref[1:2, :] = picked


def row_stats(pieces, head, other_head, wanted):
    sizes = [piece.shape[0] for piece in pieces]
    rows, (vocab, width) = sum(sizes), head.shape
    slabs = width // SLAB
    in_vmem, anywhere = pl.BlockSpec(memory_space=pltpu.VMEM), pl.BlockSpec(memory_space=pl.ANY)
    return pl.pallas_call(
        functools.partial(row_stats_kernel, sizes),
        out_shape=jax.ShapeDtypeStruct((2, rows), jnp.float32),
        in_specs=[in_vmem] + [anywhere] * (len(pieces) + 2),
        out_specs=in_vmem,
        scratch_shapes=[
            pltpu.VMEM((slabs, rows, SLAB), jnp.bfloat16),
            pltpu.VMEM((SLOTS, vocab, SLAB), jnp.bfloat16),
            pltpu.VMEM((2, vocab, rows), jnp.float32),
            pltpu.SemaphoreType.DMA((len(pieces), slabs)),
            pltpu.SemaphoreType.DMA((SLOTS,)),
        ],
        compiler_params=pltpu.CompilerParams(vmem_limit_bytes=50 * 2**20),
        cost_estimate=pl.CostEstimate(
            flops=4 * max(rows, 256) * width * vocab, bytes_accessed=4 * vocab * width, transcendentals=2 * rows * vocab
        ),
        name=f"row_stats_{rows}",
    )(wanted, *pieces, head, other_head)


def shards(hidden, head, token_ids):
    rows = hidden.shape[0]
    vocab = head.shape[0]
    me = lax.axis_index(AXES)
    partner = me ^ 16

    other_head = to_partner(head)
    plane = around(around(hidden, FIRST), SECOND)
    left, right = send(plane, THIRD, AHEAD), send(plane, THIRD, BEHIND)

    started, arrives = (lax.dynamic_index_in_dim(jnp.asarray(t), me, 0, keepdims=False) for t in arrival_tables())
    tokens = token_ids.reshape(-1, rows)[started].reshape(1, -1)
    wanted = jnp.concatenate([tokens - me * vocab, tokens - partner * vocab], axis=0)

    span = plane.shape[0]
    half = span // 2
    first = row_stats([plane], head, other_head, wanted[:, :span])
    left, right, first = together(left, right, first)
    far = [send(left[:half], THIRD, AHEAD), send(right[half:], THIRD, BEHIND)]
    second = row_stats([left, right], head, other_head, wanted[:, span : 3 * span])
    far[0], far[1], second = together(*far, second)
    third = row_stats(far, head, other_head, wanted[:, 3 * span :])
    spread, picked = jnp.concatenate([first, second, third], axis=1).reshape(2, 64, rows)
    stats = jnp.concatenate([spread, picked], axis=1)[arrives]

    groups = [[device(z, c, y, x) for z in range(4) for y in range(4) for x in range(4)] for c in range(2)]
    arrived = lax.all_to_all(stats, AXES, 0, 0, tiled=True, axis_index_groups=groups)
    spread, picked = arrived[:, :rows], jnp.sum(arrived[:, rows:], axis=0)
    top = jnp.max(spread, axis=0)
    return picked - top - jnp.log(jnp.sum(jnp.exp(spread - top[None, :]), axis=0))


def solution(mesh):
    in_specs = (P(AXES, None), P(AXES, None), P())
    return jax.shard_map(shards, mesh=mesh, in_specs=in_specs, out_specs=P(AXES), check_vma=False)
```

```python
import functools

import jax
import jax.numpy as jnp
import numpy as np
from jax import lax
from jax.experimental import pallas as pl
from jax.experimental.pallas import tpu as pltpu
from jax.sharding import PartitionSpec as P

AXES = ("replica", "tp")
FIRST, SECOND, THIRD = ("y", "x"), ("x", "z"), ("z", "y")
AHEAD, BEHIND, ACROSS = (1, -1), (-1, 1), (2, 2)
SLAB, SLOTS = 2048, 3


def device(z, core, y, x):
    return ((z % 4) * 2 + core) * 16 + (y % 4) * 4 + (x % 4)


def everyone():
    return [(z, c, y, x) for z in range(4) for c in range(2) for y in range(4) for x in range(4)]


def moved(z, c, y, x, dims, hops):
    to = {"z": z, "y": y, "x": x}
    to[dims[c]] += hops[c]
    return to["z"] % 4, c, to["y"] % 4, to["x"] % 4


def arrival_tables():
    started = np.zeros((128, 64), np.int32)
    arrives = np.zeros((128, 64), np.int32)
    back = [(0, 0), BEHIND, AHEAD, ACROSS]
    order = [half * 8 + n for half in (0, 1, 2, 5, 3, 4, 6, 7) for n in range(8)]
    for me in everyone():
        for place, block in enumerate(order):
            at = me
            for dims, slot in ((THIRD, block // 16), (SECOND, block // 4 % 4), (FIRST, block % 4)):
                at = moved(*at, dims, back[slot])
            z, _, y, x = at
            started[device(*me), place] = device(*at)
            arrives[device(*me), z * 16 + y * 4 + x] = place
    return started, arrives


def send(block, dims, hops):
    pairs = [(device(*me), device(*moved(*me, dims, hops))) for me in everyone()]
    return lax.ppermute(block, AXES, pairs)


def to_partner(block):
    pairs = [(device(z, c, y, x), device(z, 1 - c, y, x)) for z, c, y, x in everyone()]
    return lax.ppermute(block, AXES, pairs)


def around(block, dims):
    return [block] + [send(block, dims, hops) for hops in (AHEAD, BEHIND, ACROSS)]


def together(*values):
    return lax.optimization_barrier(values)


def row_stats_kernel(sizes, wanted_ref, *refs):
    pieces = refs[: len(sizes)]
    mine_ref, other_ref, out_ref, rows_ref, slab_ref, logits_ref, row_sems, slab_sems = refs[len(sizes) :]
    width = mine_ref.shape[1]
    slabs = width // SLAB

    def fetch_rows(n):
        start, copies = 0, []
        for k, (size, piece) in enumerate(zip(sizes, pieces)):
            source = piece.at[:, pl.ds(n * SLAB, SLAB)]
            copies.append(pltpu.make_async_copy(source, rows_ref.at[n, pl.ds(start, size)], row_sems.at[k, n]))
            start += size
        return copies

    def fetch_slab(head_ref, n, slot):
        source = head_ref.at[:, pl.ds(pl.multiple_of(n * SLAB, SLAB), SLAB)]
        return pltpu.make_async_copy(source, slab_ref.at[slot], slab_sems.at[slot])

    for n in range(slabs):
        if n < SLOTS - 1:
            fetch_slab(mine_ref, n, n).start()
        for copy in fetch_rows(n):
            copy.start()

    logits_ref[...] = jnp.zeros_like(logits_ref)
    for half, head_ref in enumerate((mine_ref, other_ref)):

        def step(n, _):
            turn = half * slabs + n
            slot = lax.rem(turn, SLOTS)
            ahead = n + SLOTS - 1
            free = lax.rem(turn + SLOTS - 1, SLOTS)

            @pl.when(ahead < slabs)
            def _():
                fetch_slab(head_ref, ahead, free).start()

            if half == 0:

                @pl.when(ahead >= slabs)
                def _():
                    fetch_slab(other_ref, ahead - slabs, free).start()

                start = 0
                for k, (size, piece) in enumerate(zip(sizes, pieces)):
                    source = piece.at[:, pl.ds(pl.multiple_of(n * SLAB, SLAB), SLAB)]
                    pltpu.make_async_copy(source, rows_ref.at[n, pl.ds(start, size)], row_sems.at[k, n]).wait()
                    start += size

            fetch_slab(head_ref, n, slot).wait()
            logits_ref[half] += lax.dot_general(
                slab_ref[slot], rows_ref[n], (((1,), (1,)), ((), ())), preferred_element_type=jnp.float32
            )
            return 0

        lax.fori_loop(0, slabs, step, 0)

    top = jnp.maximum(
        jnp.max(logits_ref[0], axis=0, keepdims=True), jnp.max(logits_ref[1], axis=0, keepdims=True)
    )
    entry = lax.broadcasted_iota(jnp.int32, logits_ref.shape[1:], 0)
    total, picked = jnp.zeros_like(top), jnp.zeros_like(top)
    for half in range(2):
        logits = logits_ref[half]
        total += jnp.sum(jnp.exp(logits - top), axis=0, keepdims=True)
        hit = entry == wanted_ref[half : half + 1, :]
        picked += jnp.sum(jnp.where(hit, logits, 0.0), axis=0, keepdims=True)
    out_ref[0:1, :] = top + jnp.log(total)
    out_ref[1:2, :] = picked


def row_stats(pieces, head, other_head, wanted):
    sizes = [piece.shape[0] for piece in pieces]
    rows, (vocab, width) = sum(sizes), head.shape
    slabs = width // SLAB
    in_vmem, anywhere = pl.BlockSpec(memory_space=pltpu.VMEM), pl.BlockSpec(memory_space=pl.ANY)
    return pl.pallas_call(
        functools.partial(row_stats_kernel, sizes),
        out_shape=jax.ShapeDtypeStruct((2, rows), jnp.float32),
        in_specs=[in_vmem] + [anywhere] * (len(pieces) + 2),
        out_specs=in_vmem,
        scratch_shapes=[
            pltpu.VMEM((slabs, rows, SLAB), jnp.bfloat16),
            pltpu.VMEM((SLOTS, vocab, SLAB), jnp.bfloat16),
            pltpu.VMEM((2, vocab, rows), jnp.float32),
            pltpu.SemaphoreType.DMA((len(pieces), slabs)),
            pltpu.SemaphoreType.DMA((SLOTS,)),
        ],
        compiler_params=pltpu.CompilerParams(vmem_limit_bytes=50 * 2**20),
        cost_estimate=pl.CostEstimate(
            flops=4 * max(rows, 256) * width * vocab, bytes_accessed=4 * vocab * width, transcendentals=2 * rows * vocab
        ),
        name=f"row_stats_{rows}",
    )(wanted, *pieces, head, other_head)


def shards(hidden, head, token_ids):
    rows = hidden.shape[0]
    vocab = head.shape[0]
    me = lax.axis_index(AXES)
    partner = me ^ 16

    other_head = to_partner(head)
    line = jnp.concatenate(around(hidden, FIRST), axis=0)
    lines = around(line, SECOND)
    top, bottom = jnp.concatenate(lines[:2], axis=0), jnp.concatenate(lines[2:], axis=0)
    left_top = send(top, THIRD, AHEAD)
    right_bottom = send(bottom, THIRD, BEHIND)
    left_bottom = send(bottom, THIRD, AHEAD)
    right_top = send(top, THIRD, BEHIND)
    far = [send(left_top, THIRD, AHEAD), send(right_bottom, THIRD, BEHIND)]

    started, arrives = (lax.dynamic_index_in_dim(jnp.asarray(t), me, 0, keepdims=False) for t in arrival_tables())
    tokens = token_ids.reshape(-1, rows)[started].reshape(1, -1)
    wanted = jnp.concatenate([tokens - me * vocab, tokens - partner * vocab], axis=0)

    half = wanted.shape[1] // 2
    first = row_stats([top, bottom, left_top, right_bottom], head, other_head, wanted[:, :half])
    *rest, first = together(left_bottom, right_top, *far, first)
    second = row_stats(rest, head, other_head, wanted[:, half:])
    spread, picked = jnp.concatenate([first, second], axis=1).reshape(2, 64, rows)
    stats = jnp.concatenate([spread, picked], axis=1)[arrives]

    groups = [[device(z, c, y, x) for z in range(4) for y in range(4) for x in range(4)] for c in range(2)]
    arrived = lax.all_to_all(stats, AXES, 0, 0, tiled=True, axis_index_groups=groups)
    spread, picked = arrived[:, :rows], jnp.sum(arrived[:, rows:], axis=0)
    top = jnp.max(spread, axis=0)
    return picked - top - jnp.log(jnp.sum(jnp.exp(spread - top[None, :]), axis=0))


def solution(mesh):
    in_specs = (P(AXES, None), P(AXES, None), P())
    return jax.shard_map(shards, mesh=mesh, in_specs=in_specs, out_specs=P(AXES), check_vma=False)
```

```python
import functools

import jax
import jax.numpy as jnp
import numpy as np
from jax import lax
from jax.experimental import pallas as pl
from jax.experimental.pallas import tpu as pltpu
from jax.sharding import PartitionSpec as P

AXES = ("replica", "tp")
FIRST, SECOND, THIRD = ("y", "x"), ("x", "z"), ("z", "y")
AHEAD, BEHIND, ACROSS = (1, -1), (-1, 1), (2, 2)
SLAB, SLOTS = 2048, 3


def device(z, core, y, x):
    return ((z % 4) * 2 + core) * 16 + (y % 4) * 4 + (x % 4)


def everyone():
    return [(z, c, y, x) for z in range(4) for c in range(2) for y in range(4) for x in range(4)]


def moved(z, c, y, x, dims, hops):
    to = {"z": z, "y": y, "x": x}
    to[dims[c]] += hops[c]
    return to["z"] % 4, c, to["y"] % 4, to["x"] % 4


def arrival_tables():
    started = np.zeros((128, 64), np.int32)
    arrives = np.zeros((128, 64), np.int32)
    back = [(0, 0), BEHIND, AHEAD, ACROSS]
    order = [half * 8 + n for half in (0, 1, 2, 5, 3, 4, 6, 7) for n in range(8)]
    for me in everyone():
        for place, block in enumerate(order):
            at = me
            for dims, slot in ((THIRD, block // 16), (SECOND, block // 4 % 4), (FIRST, block % 4)):
                at = moved(*at, dims, back[slot])
            z, _, y, x = at
            started[device(*me), place] = device(*at)
            arrives[device(*me), z * 16 + y * 4 + x] = place
    return started, arrives


def send(block, dims, hops):
    pairs = [(device(*me), device(*moved(*me, dims, hops))) for me in everyone()]
    return lax.ppermute(block, AXES, pairs)


def to_partner(block):
    pairs = [(device(z, c, y, x), device(z, 1 - c, y, x)) for z, c, y, x in everyone()]
    return lax.ppermute(block, AXES, pairs)


def around(block, dims):
    return [block] + [send(block, dims, hops) for hops in (AHEAD, BEHIND, ACROSS)]


def together(*values):
    return lax.optimization_barrier(values)


def row_stats_kernel(sizes, wanted_ref, *refs):
    pieces = refs[: len(sizes)]
    mine_ref, other_ref, out_ref, rows_ref, slab_ref, logits_ref, row_sems, slab_sems = refs[len(sizes) :]
    width = mine_ref.shape[1]
    slabs = width // SLAB

    def fetch_rows(n):
        start, copies = 0, []
        for k, (size, piece) in enumerate(zip(sizes, pieces)):
            source = piece.at[:, pl.ds(n * SLAB, SLAB)]
            copies.append(pltpu.make_async_copy(source, rows_ref.at[n, pl.ds(start, size)], row_sems.at[k, n]))
            start += size
        return copies

    def fetch_slab(head_ref, n, slot):
        source = head_ref.at[:, pl.ds(pl.multiple_of(n * SLAB, SLAB), SLAB)]
        return pltpu.make_async_copy(source, slab_ref.at[slot], slab_sems.at[slot])

    for n in range(slabs):
        if n < SLOTS - 1:
            fetch_slab(mine_ref, n, n).start()
        for copy in fetch_rows(n):
            copy.start()

    logits_ref[...] = jnp.zeros_like(logits_ref)
    for half, head_ref in enumerate((mine_ref, other_ref)):

        def step(n, _):
            turn = half * slabs + n
            slot = lax.rem(turn, SLOTS)
            ahead = n + SLOTS - 1
            free = lax.rem(turn + SLOTS - 1, SLOTS)

            @pl.when(ahead < slabs)
            def _():
                fetch_slab(head_ref, ahead, free).start()

            if half == 0:

                @pl.when(ahead >= slabs)
                def _():
                    fetch_slab(other_ref, ahead - slabs, free).start()

                start = 0
                for k, (size, piece) in enumerate(zip(sizes, pieces)):
                    source = piece.at[:, pl.ds(pl.multiple_of(n * SLAB, SLAB), SLAB)]
                    pltpu.make_async_copy(source, rows_ref.at[n, pl.ds(start, size)], row_sems.at[k, n]).wait()
                    start += size

            fetch_slab(head_ref, n, slot).wait()
            logits_ref[half] += lax.dot_general(
                slab_ref[slot], rows_ref[n], (((1,), (1,)), ((), ())), preferred_element_type=jnp.float32
            )
            return 0

        lax.fori_loop(0, slabs, step, 0)

    top = jnp.maximum(
        jnp.max(logits_ref[0], axis=0, keepdims=True), jnp.max(logits_ref[1], axis=0, keepdims=True)
    )
    entry = lax.broadcasted_iota(jnp.int32, logits_ref.shape[1:], 0)
    total, picked = jnp.zeros_like(top), jnp.zeros_like(top)
    for half in range(2):
        logits = logits_ref[half]
        total += jnp.sum(jnp.exp(logits - top), axis=0, keepdims=True)
        hit = entry == wanted_ref[half : half + 1, :]
        picked += jnp.sum(jnp.where(hit, logits, 0.0), axis=0, keepdims=True)
    out_ref[0:1, :] = top + jnp.log(total)
    out_ref[1:2, :] = picked


def row_stats(pieces, head, other_head, wanted):
    sizes = [piece.shape[0] for piece in pieces]
    rows, (vocab, width) = sum(sizes), head.shape
    slabs = width // SLAB
    in_vmem, anywhere = pl.BlockSpec(memory_space=pltpu.VMEM), pl.BlockSpec(memory_space=pl.ANY)
    return pl.pallas_call(
        functools.partial(row_stats_kernel, sizes),
        out_shape=jax.ShapeDtypeStruct((2, rows), jnp.float32),
        in_specs=[in_vmem] + [anywhere] * (len(pieces) + 2),
        out_specs=in_vmem,
        scratch_shapes=[
            pltpu.VMEM((slabs, rows, SLAB), jnp.bfloat16),
            pltpu.VMEM((SLOTS, vocab, SLAB), jnp.bfloat16),
            pltpu.VMEM((2, vocab, rows), jnp.float32),
            pltpu.SemaphoreType.DMA((len(pieces), slabs)),
            pltpu.SemaphoreType.DMA((SLOTS,)),
        ],
        compiler_params=pltpu.CompilerParams(vmem_limit_bytes=50 * 2**20),
        cost_estimate=pl.CostEstimate(
            flops=4 * max(rows, 256) * width * vocab, bytes_accessed=4 * vocab * width, transcendentals=2 * rows * vocab
        ),
        name=f"row_stats_{rows}",
    )(wanted, *pieces, head, other_head)


def shards(hidden, head, token_ids):
    rows = hidden.shape[0]
    vocab = head.shape[0]
    me = lax.axis_index(AXES)
    partner = me ^ 16

    other_head = to_partner(head)
    line = jnp.concatenate(around(hidden, FIRST), axis=0)
    behind, ahead = send(line, SECOND, AHEAD), send(line, SECOND, BEHIND)
    split = line.shape[0] // 2
    across = [send(behind[:split], SECOND, AHEAD), send(ahead[split:], SECOND, BEHIND)]
    top, across = jnp.concatenate([line, behind], axis=0), jnp.concatenate(across, axis=0)
    bottom = jnp.concatenate([ahead, across], axis=0)
    left_top = send(top, THIRD, AHEAD)
    right_bottom = [send(ahead, THIRD, BEHIND), send(across, THIRD, BEHIND)]
    left_bottom = send(bottom, THIRD, AHEAD)
    late_top, _ = together(top, across)
    right_top = send(late_top, THIRD, BEHIND)
    far = [send(left_top, THIRD, AHEAD)] + [send(part, THIRD, BEHIND) for part in right_bottom]

    started, arrives = (lax.dynamic_index_in_dim(jnp.asarray(t), me, 0, keepdims=False) for t in arrival_tables())
    tokens = token_ids.reshape(-1, rows)[started].reshape(1, -1)
    wanted = jnp.concatenate([tokens - me * vocab, tokens - partner * vocab], axis=0)

    half = wanted.shape[1] // 2
    first = row_stats([top, ahead, across, left_top, *right_bottom], head, other_head, wanted[:, :half])
    *rest, first = together(left_bottom, right_top, *far, first)
    second = row_stats(rest, head, other_head, wanted[:, half:])
    spread, picked = jnp.concatenate([first, second], axis=1).reshape(2, 64, rows)
    stats = jnp.concatenate([spread, picked], axis=1)[arrives]

    groups = [[device(z, c, y, x) for z in range(4) for y in range(4) for x in range(4)] for c in range(2)]
    arrived = lax.all_to_all(stats, AXES, 0, 0, tiled=True, axis_index_groups=groups)
    spread, picked = arrived[:, :rows], jnp.sum(arrived[:, rows:], axis=0)
    top = jnp.max(spread, axis=0)
    return picked - top - jnp.log(jnp.sum(jnp.exp(spread - top[None, :]), axis=0))


def solution(mesh):
    in_specs = (P(AXES, None), P(AXES, None), P())
    return jax.shard_map(shards, mesh=mesh, in_specs=in_specs, out_specs=P(AXES), check_vma=False)
```

```python
import functools

import jax
import jax.numpy as jnp
import numpy as np
from jax import lax
from jax.experimental import pallas as pl
from jax.experimental.pallas import tpu as pltpu
from jax.sharding import PartitionSpec as P

AXES = ("replica", "tp")
FIRST, SECOND, THIRD = ("y", "x"), ("x", "z"), ("z", "y")
AHEAD, BEHIND, ACROSS = (1, -1), (-1, 1), (2, 2)
SLAB, SLOTS = 2048, 3


def device(z, core, y, x):
    return ((z % 4) * 2 + core) * 16 + (y % 4) * 4 + (x % 4)


def everyone():
    return [(z, c, y, x) for z in range(4) for c in range(2) for y in range(4) for x in range(4)]


def moved(z, c, y, x, dims, hops):
    to = {"z": z, "y": y, "x": x}
    to[dims[c]] += hops[c]
    return to["z"] % 4, c, to["y"] % 4, to["x"] % 4


def arrival_tables():
    started = np.zeros((128, 64), np.int32)
    arrives = np.zeros((128, 64), np.int32)
    back = [(0, 0), BEHIND, AHEAD, ACROSS]
    order = [half * 8 + n for half in (0, 1, 2, 5, 3, 4, 6, 7) for n in range(8)]
    for me in everyone():
        for place, block in enumerate(order):
            at = me
            for dims, slot in ((THIRD, block // 16), (SECOND, block // 4 % 4), (FIRST, block % 4)):
                at = moved(*at, dims, back[slot])
            z, _, y, x = at
            started[device(*me), place] = device(*at)
            arrives[device(*me), z * 16 + y * 4 + x] = place
    return started, arrives


def send(block, dims, hops):
    pairs = [(device(*me), device(*moved(*me, dims, hops))) for me in everyone()]
    return lax.ppermute(block, AXES, pairs)


def to_partner(block):
    pairs = [(device(z, c, y, x), device(z, 1 - c, y, x)) for z, c, y, x in everyone()]
    return lax.ppermute(block, AXES, pairs)


def around(block, dims):
    return [block] + [send(block, dims, hops) for hops in (AHEAD, BEHIND, ACROSS)]


def together(*values):
    return lax.optimization_barrier(values)


def row_stats_kernel(sizes, held, wanted_ref, *refs):
    pieces = refs[: len(sizes)]
    mine_ref, other_ref, first, second, rows_ref, slab_ref, logits_ref, row_sems, slab_sems, kept_sem = refs[len(sizes) :]
    kept_ref, out_ref = (first, second) if held else (second, first)
    width = mine_ref.shape[1]
    slabs = width // SLAB

    def fetch_rows(n):
        start, copies = 0, []
        for k, (size, piece) in enumerate(zip(sizes, pieces)):
            source = piece.at[:, pl.ds(n * SLAB, SLAB)]
            copies.append(pltpu.make_async_copy(source, rows_ref.at[n, pl.ds(start, size)], row_sems.at[k, n]))
            start += size
        return copies

    def fetch_slab(head_ref, n, slot):
        source = head_ref.at[:, pl.ds(pl.multiple_of(n * SLAB, SLAB), SLAB)]
        return pltpu.make_async_copy(source, slab_ref.at[slot], slab_sems.at[slot])

    for n in range(slabs):
        if (1 if held else 0) <= n < SLOTS - 1:
            fetch_slab(mine_ref, n, n).start()
        for copy in fetch_rows(n):
            copy.start()

    logits_ref[...] = jnp.zeros_like(logits_ref)
    for half, head_ref in enumerate((mine_ref, other_ref)):

        def step(n, _, kept=False):
            turn = half * slabs + n
            slot = lax.rem(turn, SLOTS)
            ahead = n + SLOTS - 1
            free = lax.rem(turn + SLOTS - 1, SLOTS)

            @pl.when(ahead < slabs)
            def _():
                fetch_slab(head_ref, ahead, free).start()

            if half == 0:

                @pl.when(ahead >= slabs)
                def _():
                    fetch_slab(other_ref, ahead - slabs, free).start()

                start = 0
                for k, (size, piece) in enumerate(zip(sizes, pieces)):
                    source = piece.at[:, pl.ds(pl.multiple_of(n * SLAB, SLAB), SLAB)]
                    pltpu.make_async_copy(source, rows_ref.at[n, pl.ds(start, size)], row_sems.at[k, n]).wait()
                    start += size

            if not kept:
                fetch_slab(head_ref, n, slot).wait()
            logits_ref[half] += lax.dot_general(
                kept_ref[...] if kept else slab_ref[slot], rows_ref[n], (((1,), (1,)), ((), ())), preferred_element_type=jnp.float32
            )
            return 0

        keep = pltpu.make_async_copy(mine_ref.at[:, pl.ds(0, SLAB)], kept_ref, kept_sem)
        if held and half == 0:
            lax.fori_loop(0, 1, functools.partial(step, kept=True), 0)
            lax.fori_loop(1, slabs, step, 0)
        else:
            if half == 1 and not held:
                keep.start()
            lax.fori_loop(0, slabs, step, 0)
            if half == 1 and not held:
                keep.wait()

    top = jnp.maximum(
        jnp.max(logits_ref[0], axis=0, keepdims=True), jnp.max(logits_ref[1], axis=0, keepdims=True)
    )
    entry = lax.broadcasted_iota(jnp.int32, logits_ref.shape[1:], 0)
    total, picked = jnp.zeros_like(top), jnp.zeros_like(top)
    for half in range(2):
        logits = logits_ref[half]
        total += jnp.sum(jnp.exp(logits - top), axis=0, keepdims=True)
        hit = entry == wanted_ref[half : half + 1, :]
        picked += jnp.sum(jnp.where(hit, logits, 0.0), axis=0, keepdims=True)
    out_ref[0:1, :] = top + jnp.log(total)
    out_ref[1:2, :] = picked


def row_stats(pieces, head, other_head, wanted, kept=None):
    sizes = [piece.shape[0] for piece in pieces]
    rows, (vocab, width) = sum(sizes), head.shape
    slabs = width // SLAB
    in_vmem, anywhere = pl.BlockSpec(memory_space=pltpu.VMEM), pl.BlockSpec(memory_space=pl.ANY)
    return pl.pallas_call(
        functools.partial(row_stats_kernel, sizes, kept is not None),
        out_shape=[jax.ShapeDtypeStruct((2, rows), jnp.float32)]
        + ([] if kept is not None else [pltpu.VMEM((vocab, SLAB), jnp.bfloat16)]),
        in_specs=[in_vmem] + [anywhere] * (len(pieces) + 2) + ([] if kept is None else [in_vmem]),
        out_specs=[in_vmem] * (2 if kept is None else 1),
        scratch_shapes=[
            pltpu.VMEM((slabs, rows, SLAB), jnp.bfloat16),
            pltpu.VMEM((SLOTS, vocab, SLAB), jnp.bfloat16),
            pltpu.VMEM((2, vocab, rows), jnp.float32),
            pltpu.SemaphoreType.DMA((len(pieces), slabs)),
            pltpu.SemaphoreType.DMA((SLOTS,)),
            pltpu.SemaphoreType.DMA,
        ],
        compiler_params=pltpu.CompilerParams(vmem_limit_bytes=44 * 2**20),
        cost_estimate=pl.CostEstimate(
            flops=4 * max(rows, 256) * width * vocab, bytes_accessed=4 * vocab * width, transcendentals=2 * rows * vocab
        ),
        name=f"row_stats_{rows}",
    )(wanted, *pieces, head, other_head, *([] if kept is None else [kept]))


def shards(hidden, head, token_ids):
    rows = hidden.shape[0]
    vocab = head.shape[0]
    me = lax.axis_index(AXES)
    partner = me ^ 16

    other_head = to_partner(head)
    line = jnp.concatenate(around(hidden, FIRST), axis=0)
    behind, ahead = send(line, SECOND, AHEAD), send(line, SECOND, BEHIND)
    split = line.shape[0] // 2
    across = [send(behind[:split], SECOND, AHEAD), send(ahead[split:], SECOND, BEHIND)]
    top, across = jnp.concatenate([line, behind], axis=0), jnp.concatenate(across, axis=0)
    bottom = jnp.concatenate([ahead, across], axis=0)
    left_top = send(top, THIRD, AHEAD)
    right_bottom = [send(ahead, THIRD, BEHIND), send(across, THIRD, BEHIND)]
    left_bottom = send(bottom, THIRD, AHEAD)
    late_top, _ = together(top, across)
    right_top = send(late_top, THIRD, BEHIND)
    far = [send(left_top, THIRD, AHEAD)] + [send(part, THIRD, BEHIND) for part in right_bottom]

    started, arrives = (lax.dynamic_index_in_dim(jnp.asarray(t), me, 0, keepdims=False) for t in arrival_tables())
    tokens = token_ids.reshape(-1, rows)[started].reshape(1, -1)
    wanted = jnp.concatenate([tokens - me * vocab, tokens - partner * vocab], axis=0)

    half = wanted.shape[1] // 2
    first, kept = row_stats([top, ahead, across, left_top, *right_bottom], head, other_head, wanted[:, :half])
    *rest, first = together(left_bottom, right_top, *far, first)
    (second,) = row_stats(rest, head, other_head, wanted[:, half:], kept)
    spread, picked = jnp.concatenate([first, second], axis=1).reshape(2, 64, rows)
    stats = jnp.concatenate([spread, picked], axis=1)[arrives]

    groups = [[device(z, c, y, x) for z in range(4) for y in range(4) for x in range(4)] for c in range(2)]
    arrived = lax.all_to_all(stats, AXES, 0, 0, tiled=True, axis_index_groups=groups)
    spread, picked = arrived[:, :rows], jnp.sum(arrived[:, rows:], axis=0)
    top = jnp.max(spread, axis=0)
    return picked - top - jnp.log(jnp.sum(jnp.exp(spread - top[None, :]), axis=0))


def solution(mesh):
    in_specs = (P(AXES, None), P(AXES, None), P())
    return jax.shard_map(shards, mesh=mesh, in_specs=in_specs, out_specs=P(AXES), check_vma=False)
```
